32 devices in a mesh: tiles: 16 (over z, x, core), strip: 2 (over y).
Axes of the slice: x: 2, y: 2, z: 4, core: 2. Of those that a mesh axis runs over, the one named last changes fastest.
Arguments:
- fields: float32 [16, 2, 3, 3, 4, 8100], P('tiles', 'strip'), may hold values from -6 to 6
- wet_land: int32 [16, 2, 3, 8100], P('tiles', 'strip'), may hold values from 0 to 1, as said below
- links: int32 [16, 2, 3, 4, 4], P('tiles', 'strip'), may hold values from -1 to 3, as said below
- surface_diagonal: float32 [16, 2, 3, 8100], P('tiles', 'strip'), may hold values from 0.25 to 2
- spread: float32 [3, 4], replicated, may hold values from 0.02 to 0.2
- mixing: float32 [4], replicated, may hold values from 0.02 to 0.2
- thickness: float32 [4], replicated, may hold values from 0.5 to 2
Outputs:
- adjoint_fields: float32 [16, 2, 3, 3, 4, 8100], P('tiles', 'strip')
- surface_solution: float32 [16, 2, 3, 8100], P('tiles', 'strip')
- surface_residual: float32 [16, 2, 3, 8100], P('tiles', 'strip')
The draws below stay inside these ranges and needn't reach their ends.
Inputs may be any that keep to these rules, and one draw needn't show every extreme that they name: wet_land is 1 on most cells of the first 1 to 3 slots of each device and 0 on all cells of its other slots. Offsets dt and ds are -1, 0 or 1; on the west and east sides dt is -1 and 1, on the south and north sides ds is -1 and 1; a partner slot is -1 or a slot that holds wet cells; links are mutual: side e of slot k pairs with side e XOR 1 of its partner, whose entry points back with opposite offsets and rotation code (4 - code) mod 4; an empty slot has no links; rotation codes are 0 to 3.
All inputs are finite; a program needn't handle non-finite values.
Results may differ from the reference program's by a relative error of at most 0.00027.
Values sent between devices are 32-bit elements; how exact they have to be, the bound alone decides.
A program may use at most 64 MiB of HBM per device.

```python
import math
import jax
import jax.numpy as jnp
import numpy as np
from jax import lax

TILE = 90
SLOTS = 3
FIELDS = 3
LEVELS = 4
ITERS = 2
CELLS = 8100
TILE_GROUPS = 16
STRIP_GROUPS = 2


def wet_counts(key):
    return jax.random.randint(jax.random.fold_in(key, 11), (TILE_GROUPS, STRIP_GROUPS), 1, SLOTS + 1)


def live_slots(key):
    counts = wet_counts(key)
    return jnp.arange(SLOTS, dtype=jnp.int32)[None, None, :] < counts[:, :, None]


def draw_wet_land(key, part):
    live = live_slots(key)
    ocean = jax.random.randint(jax.random.fold_in(key, 13), (TILE_GROUPS, STRIP_GROUPS, SLOTS, CELLS), 0, 8) != 0
    return (live[..., None] & ocean).astype(jnp.int32)


def slot_orders(key):
    scores = jax.random.randint(key, (TILE_GROUPS, STRIP_GROUPS, SLOTS), 0, 1 << 20) * SLOTS
    scores = scores + jnp.arange(SLOTS, dtype=jnp.int32)[None, None, :]
    order = jnp.argsort(scores, axis=-1).astype(jnp.int32)
    inverse = jnp.argsort(order, axis=-1).astype(jnp.int32)
    return (order, inverse)


def entry_table(group_shift, strip_shift, partner, code):
    shape = (TILE_GROUPS, STRIP_GROUPS, SLOTS)
    return jnp.stack([jnp.broadcast_to(group_shift, shape), jnp.broadcast_to(strip_shift, shape), jnp.broadcast_to(partner, shape), jnp.broadcast_to(code, shape)], axis=-1).astype(jnp.int32)


def draw_links(key, part):
    live = live_slots(key)
    shape = (TILE_GROUPS, STRIP_GROUPS, SLOTS)
    group_ids = jnp.arange(TILE_GROUPS, dtype=jnp.int32)[:, None, None]
    strip_ids = jnp.arange(STRIP_GROUPS, dtype=jnp.int32)[None, :, None]
    slot_ids = jnp.arange(SLOTS, dtype=jnp.int32)[None, None, :]
    east_shift = jax.random.randint(jax.random.fold_in(key, 21), (TILE_GROUPS,), -1, 2)
    east_order, east_inverse = slot_orders(jax.random.fold_in(key, 22))
    east_code = jax.random.randint(jax.random.fold_in(key, 23), shape, 0, 4)
    east_cut = jax.random.randint(jax.random.fold_in(key, 24), shape, 0, 8) == 0
    east_group = (group_ids + 1) % TILE_GROUPS
    east_strip = (strip_ids + east_shift[:, None, None]) % STRIP_GROUPS
    east_live = live & live[east_group, east_strip, east_order] & jnp.logical_not(east_cut)
    east_entry = entry_table(1, east_shift[:, None, None], jnp.where(east_live, east_order, -1), east_code)
    from_group = (group_ids - 1) % TILE_GROUPS
    west_shift = east_shift[from_group]
    from_strip = (strip_ids - west_shift) % STRIP_GROUPS
    from_slot = east_inverse[from_group, from_strip, slot_ids]
    west_live = east_live[from_group, from_strip, from_slot]
    west_code = (4 - east_code[from_group, from_strip, from_slot]) % 4
    west_entry = entry_table(-1, -west_shift, jnp.where(west_live, from_slot, -1), west_code)
    north_shift = jax.random.randint(jax.random.fold_in(key, 31), (STRIP_GROUPS,), -1, 2)
    north_order, north_inverse = slot_orders(jax.random.fold_in(key, 32))
    north_code = jax.random.randint(jax.random.fold_in(key, 33), shape, 0, 4)
    north_cut = jax.random.randint(jax.random.fold_in(key, 34), shape, 0, 8) == 0
    north_group = (group_ids + north_shift[None, :, None]) % TILE_GROUPS
    north_strip = (strip_ids + 1) % STRIP_GROUPS
    north_live = live & live[north_group, north_strip, north_order] & jnp.logical_not(north_cut)
    north_entry = entry_table(north_shift[None, :, None], 1, jnp.where(north_live, north_order, -1), north_code)
    below_strip = (strip_ids - 1) % STRIP_GROUPS
    south_shift = north_shift[below_strip]
    below_group = (group_ids - south_shift) % TILE_GROUPS
    below_slot = north_inverse[below_group, below_strip, slot_ids]
    south_live = north_live[below_group, below_strip, below_slot]
    south_code = (4 - north_code[below_group, below_strip, below_slot]) % 4
    south_entry = entry_table(-south_shift, -1, jnp.where(south_live, below_slot, -1), south_code)
    return jnp.stack([west_entry, east_entry, south_entry, north_entry], axis=3)


def steps_of(stream_key, dims, cuts, low, largest):
    def one(position, blocks):
        draws = jax.random.uniform(jax.random.fold_in(jax.random.fold_in(stream_key, 6), position), (blocks,), jnp.float32, low / len(cuts), largest / len(cuts))
        return jnp.repeat(jnp.exp(draws), dims[position] // blocks).reshape((-1,) + (1,) * (len(dims) - position - 1))

    level = one(*cuts[0])
    for cut in cuts[1:]:
        level = level * one(*cut)
    return level


def scatter_about(key, extent, scale, bound, cuts=(), kind=jnp.bfloat16):
    gain = steps_of(key, extent, cuts, -0.22, 0.18) if cuts else 1.0
    values = jax.random.normal(key, extent, jnp.float32) * scale * gain
    return jnp.minimum(jnp.maximum(values, -bound), bound).astype(kind)


def setup_inputs(seed: int = 0) -> dict:
    key_list = jax.random.split(jax.random.key(seed), 8)
    return {
        "fields": scatter_about(key_list[0], (TILE_GROUPS, STRIP_GROUPS, SLOTS, FIELDS, LEVELS, CELLS), 1.0, 6.0, ((0, 16), (1, 2)), jnp.float32),
        "wet_land": draw_wet_land(jax.random.fold_in(key_list[7], 71), 0),
        "links": draw_links(jax.random.fold_in(key_list[7], 71), 0),
        "surface_diagonal": jnp.clip(0.25 + 1.75 * jax.random.uniform(key_list[3], (TILE_GROUPS, STRIP_GROUPS, SLOTS, CELLS), jnp.float32) ** steps_of(key_list[3], (TILE_GROUPS, STRIP_GROUPS, SLOTS, CELLS), ((0, 16), (1, 2)), -0.2, 0.2), 0.25, 2.0),
        "spread": jnp.clip(jnp.exp(jax.random.uniform(key_list[4], (FIELDS, LEVELS), jnp.float32, math.log(0.02), math.log(0.2))), 0.02, 0.2),
        "mixing": jnp.clip(jnp.exp(jax.random.uniform(key_list[5], (LEVELS,), jnp.float32, math.log(0.02), math.log(0.2))), 0.02, 0.2),
        "thickness": jnp.clip(jnp.exp(jax.random.uniform(key_list[6], (LEVELS,), jnp.float32, math.log(0.5), math.log(2.0))), 0.5, 2.0),
    }


OPPOSITE = np.array([1, 0, 3, 2], np.int32)


def rim_rows(values, width):
    west_rim = values[..., ::width]
    east_rim = values[..., width - 1::width]
    south_rim = values[..., :width]
    north_rim = values[..., -width:]
    return jnp.concatenate([west_rim, east_rim, south_rim, north_rim], axis=-1)


def beside_values(values, rims, width):
    cells_total = values.shape[-1]
    leading = values.shape[:-1]
    places = jnp.arange(cells_total, dtype=jnp.int32)
    column_index = places % width
    row_index = places // width
    west_full = jnp.broadcast_to(rims[..., 0, :, None], leading + (width, width)).reshape(leading + (cells_total,))
    east_full = jnp.broadcast_to(rims[..., 1, :, None], leading + (width, width)).reshape(leading + (cells_total,))
    south_full = jnp.broadcast_to(rims[..., 2, None, :], leading + (width, width)).reshape(leading + (cells_total,))
    north_full = jnp.broadcast_to(rims[..., 3, None, :], leading + (width, width)).reshape(leading + (cells_total,))
    zero_cell = jnp.zeros(leading + (1,), jnp.float32)
    zero_line = jnp.zeros(leading + (width,), jnp.float32)
    west_side = jnp.where(column_index == 0, west_full, jnp.concatenate([zero_cell, values[..., :-1]], -1))
    east_side = jnp.where(column_index == width - 1, east_full, jnp.concatenate([values[..., 1:], zero_cell], -1))
    south_side = jnp.where(row_index == 0, south_full, jnp.concatenate([zero_line, values[..., :-width]], -1))
    north_side = jnp.where(row_index == width - 1, north_full, jnp.concatenate([values[..., width:], zero_line], -1))
    return west_side, east_side, south_side, north_side


def orient(picked, links, vector):
    code = links[..., 3]
    partner = links[..., 2]
    lead = code.ndim
    extra = picked.ndim - lead
    tail_shape = code.shape + (1,) * extra
    flipped = jnp.where((code != 0).reshape(tail_shape), jnp.flip(picked, -1), picked)
    flipped = flipped * (partner >= 0).astype(jnp.float32).reshape(tail_shape)
    if vector:
        turn_shape = code.shape + (1,) * (extra - 1)
        cosine_part = ((code == 0).astype(jnp.float32) - (code == 2).astype(jnp.float32)).reshape(turn_shape)
        sine_part = ((code == 1).astype(jnp.float32) - (code == 3).astype(jnp.float32)).reshape(turn_shape)
        eastward = jnp.take(flipped, 0, axis=lead)
        northward = jnp.take(flipped, 1, axis=lead)
        scalar_part = jnp.take(flipped, 2, axis=lead)
        flipped = jnp.stack([cosine_part * eastward + sine_part * northward,
                             cosine_part * northward - sine_part * eastward, scalar_part], axis=lead)
    return jnp.moveaxis(flipped, lead - 1, -2)


def slab_step(fields, wet, rims, spread, mixing, thickness, width):
    wet_cells = wet[..., None, None, :]
    masked = fields * wet_cells
    west_side, east_side, south_side, north_side = beside_values(masked, rims, width)
    flat_term = west_side + east_side + south_side + north_side - 4.0 * masked
    above = jnp.concatenate([masked[..., 1:, :], masked[..., -1:, :]], axis=-2)
    below = jnp.concatenate([masked[..., :1, :], masked[..., :-1, :]], axis=-2)
    column_term = above + below - 2.0 * masked
    updated = wet_cells * (masked + spread[:, :, None] * flat_term + mixing[:, None] * column_term)
    flux = 0.5 * (east_side[..., 0, :, :] - west_side[..., 0, :, :] + north_side[..., 1, :, :] - south_side[..., 1, :, :])
    source = wet * jnp.sum(thickness[:, None] * flux, axis=-2)
    return updated, source


def surface_apply(values, wet, rims, diagonal, width):
    west_side, east_side, south_side, north_side = beside_values(values, rims, width)
    return wet * ((4.0 + diagonal) * values - (west_side + east_side + south_side + north_side))


def pick_global(packs, links):
    group_shift = links[..., 0]
    strip_shift = links[..., 1]
    partner = jnp.maximum(links[..., 2], 0)
    group_index = (jnp.arange(TILE_GROUPS, dtype=jnp.int32)[:, None, None, None] + group_shift) % TILE_GROUPS
    strip_index = (jnp.arange(STRIP_GROUPS, dtype=jnp.int32)[None, :, None, None] + strip_shift) % STRIP_GROUPS
    opposite = jnp.broadcast_to(jnp.asarray(OPPOSITE)[None, None, None, :], partner.shape)
    return packs[group_index, strip_index, partner, ..., opposite, :]


def reference(fields, wet_land, links, surface_diagonal, spread, mixing, thickness):
    wet = wet_land.astype(jnp.float32)
    masked = fields * wet[:, :, :, None, None, :]
    slab_packs = rim_rows(masked, TILE).reshape(masked.shape[:-1] + (4, TILE))
    slab_rims = orient(pick_global(slab_packs, links), links, True)

    def one_group(items):
        group_fields, group_wet, group_rims = items
        return slab_step(group_fields, group_wet, group_rims, spread, mixing, thickness, TILE)

    updated, source = lax.map(one_group, (fields, wet, slab_rims))

    def surface_image(values):
        packs = rim_rows(values, TILE).reshape(values.shape[:-1] + (4, TILE))
        rims = orient(pick_global(packs, links), links, False)
        return surface_apply(values, wet, rims, surface_diagonal, TILE)

    solution = jnp.zeros_like(source)
    residual = source
    direction = source
    norm_now = jnp.sum(residual * residual)
    for iteration in range(ITERS):
        image = surface_image(direction)
        alpha = norm_now / jnp.sum(direction * image)
        solution = solution + alpha * direction
        residual = residual - alpha * image
        if iteration + 1 < ITERS:
            norm_next = jnp.sum(residual * residual)
            direction = residual + (norm_next / norm_now) * direction
            norm_now = norm_next
    return updated, solution, residual
```

```python
import math

import jax
import jax.numpy as jnp
from jax import lax
from jax.experimental import pallas as pl
from jax.experimental.pallas import tpu as pltpu
from jax.sharding import PartitionSpec as P

LANES = 128
CHUNK = 1024
POS = (0, 3, 1, 2)
GROUP = 16


def offsets(size):
    return (-1, 0, 1) if size >= 3 else tuple(range(size))


def place(offset, size):
    if size >= 3:
        return offset + 1
    return offset * offset if size == 2 else 0 * offset


def roll(value, shift, axis=1):
    size = value.shape[axis]
    shift = shift % size
    return pltpu.roll(value, shift, axis) if shift else value


def build(tiles, strips, slots, fields_n, levels, cells):
    width = math.isqrt(cells)
    n_tiles = -(-cells // CHUNK) * CHUNK // LANES
    wide = n_tiles * LANES
    padded = wide + 2 * LANES
    chunks = wide // CHUNK
    steps_t, steps_s = offsets(tiles), offsets(strips)
    n_s = len(steps_s)
    n_dirs = len(steps_t) * n_s
    low = min(GROUP, tiles)
    high = tiles // low
    first = low * strips
    directions = []
    for dt in steps_t:
        for ds in steps_s:
            if dt == 0 and ds == 0:
                continue
            sides = []
            if dt == -1 or (tiles == 2 and dt):
                sides.append(0)
            if ds == -1 or (strips == 2 and ds):
                sides.append(1)
            if ds == 1:
                sides.append(2)
            if dt == 1:
                sides.append(3)
            here = place(dt, tiles) * n_s + place(ds, strips)
            back = place(-dt if tiles >= 3 else dt, tiles) * n_s + place(-ds if strips >= 3 else ds, strips)
            directions.append((dt, ds, here, back, min(sides), max(sides) + 1))

    def kernel(
        fields, wet_in, links, diag_in, spread, mixing, thick, out_f, out_x, out_r,
        fbuf, wbuf, dbuf, m_ref, w_ref, d_ref, nw_ref, ne_ref, uv_ref, s_ref, u_ref, v_ref, eb_ref, ebs_ref,
        rim_ref, rims_ref, pack1, near1, packb, nearb, pack2, near2, pack3, near3, row_ref, red_ref, red2_ref,
        in_sem, out_sem, send1, recv1, sendb, recvb, send2, recv2, send3, recv3, sendr, recvr, sendq, recvq,
    ):
        t = lax.axis_index("tiles")
        s = lax.axis_index("strip")
        copies = [
            pltpu.make_async_copy(wet_in.at[0, 0], wbuf, in_sem.at[0]),
            pltpu.make_async_copy(diag_in.at[0, 0], dbuf, in_sem.at[1]),
        ] + [pltpu.make_async_copy(fields.at[0, 0, k], fbuf.at[k], in_sem.at[2 + k]) for k in range(slots)]
        for copy in copies:
            copy.start()

        barrier = pltpu.get_barrier_semaphore()
        base = (t // low) * low
        place_t = t % low
        me_first = place_t * strips + s
        peers = 0
        for j in range(1, first):
            other = lax.rem(me_first + j, first)
            pl.semaphore_signal(
                barrier, inc=1, device_id=(base + other // strips, other % strips),
                device_id_type=pl.DeviceIdType.MESH,
            )
            peers += 1
        for j in range(1, high):
            other = lax.rem(t // low + j, high)
            pl.semaphore_signal(
                barrier, inc=1, device_id=(other * low + place_t, s), device_id_type=pl.DeviceIdType.MESH
            )
            peers += 1
        if high > 1:
            for dt, ds, here, back, lo, hi in directions:
                pl.semaphore_signal(
                    barrier, inc=1,
                    device_id=(lax.rem(t + dt + tiles, tiles), lax.rem(s + ds + strips, strips)),
                    device_id_type=pl.DeviceIdType.MESH,
                )
                peers += 1

        def exchange(pack, near, send_sem, recv_sem):
            out = []
            for dt, ds, here, back, lo, hi in directions:
                copy = pltpu.make_async_remote_copy(
                    src_ref=pack.at[pl.ds(lo, hi - lo)],
                    dst_ref=near.at[back, pl.ds(lo, hi - lo)],
                    send_sem=send_sem.at[here],
                    recv_sem=recv_sem.at[back],
                    device_id=(lax.rem(t + dt + tiles, tiles), lax.rem(s + ds + strips, strips)),
                    device_id_type=pl.DeviceIdType.MESH,
                )
                copy.start()
                out.append(copy)
            return out

        lane = lax.broadcasted_iota(jnp.int32, (1, LANES), 1)
        flip_at = jnp.where(lane < width, width - 1 - lane, lane)

        def flip(value):
            rows = value.shape[0]
            if rows < 8:
                value = jnp.concatenate([value, jnp.zeros((8 - rows, LANES), jnp.float32)], 0)
            at = jnp.broadcast_to(flip_at, value.shape)
            return jnp.take_along_axis(value, at, axis=1)[:rows]

        def extract(tile, rows):
            blank = jnp.zeros((rows, LANES), jnp.float32)
            parts_w, parts_e = [blank] * 4, [blank] * 4
            loaded = {}

            def at(n):
                if n not in loaded:
                    loaded[n] = tile(n)
                return loaded[n]

            for i in range(-1, width):
                pe = width * i + width - 1
                pw = pe + 1
                shift = (i - pe) % LANES
                turned = {}
                for n in {pe // LANES if i >= 0 else pw // LANES, pw // LANES if i + 1 < width else pe // LANES}:
                    turned[n] = roll(at(n), shift)
                if i >= 0:
                    parts_e[i % 4] = jnp.where(lane == i, turned[pe // LANES], parts_e[i % 4])
                if i + 1 < width:
                    parts_w[i % 4] = jnp.where(lane == i + 1, turned[pw // LANES], parts_w[i % 4])
            west = (parts_w[0] + parts_w[1]) + (parts_w[2] + parts_w[3])
            east = (parts_e[0] + parts_e[1]) + (parts_e[2] + parts_e[3])

            def line(start):
                a, n = start % LANES, start // LANES
                if a == 0:
                    return jnp.where(lane < width, at(n), 0.0)
                head = roll(at(n), -a)
                if a + width <= LANES:
                    return jnp.where(lane < width, head, 0.0)
                tail = roll(at(n + 1), -a)
                return jnp.where(lane < LANES - a, head, jnp.where(lane < width, tail, 0.0))

            return west, east, line(0), line(width * (width - 1))

        def insert(west, east, south, north, store):
            even = (lane & 1) == 0
            mixed = (jnp.where(even, east, west), jnp.where(even, west, east))
            tiles_of = {}

            def add(n, mask, value):
                tiles_of.setdefault(n, []).append((mask, value))

            for i in range(-1, width):
                pe = width * i + width - 1
                pw = pe + 1
                turned = roll(mixed[i % 2], (pe - i) % LANES)
                if i >= 0 and i + 1 < width and pe // LANES == pw // LANES:
                    mask = (lane == pe % LANES) | (lane == pw % LANES)
                    add(pe // LANES, mask, turned)
                else:
                    if i >= 0:
                        add(pe // LANES, lane == pe % LANES, turned)
                    if i + 1 < width:
                        add(pw // LANES, lane == pw % LANES, turned)
            extra = {}
            for start, rim in ((0, south), (width * (width - 1), north)):
                a, n = start % LANES, start // LANES
                turned = roll(rim, a)
                extra.setdefault(n, []).append(jnp.where(lane >= a, turned, 0.0) if a else turned)
                if a + width > LANES:
                    extra.setdefault(n + 1, []).append(jnp.where(lane < a + width - LANES, turned, 0.0))
            blank = jnp.zeros(west.shape, jnp.float32)
            for n in range(n_tiles):
                total = blank
                for mask, value in tiles_of.get(n, ()):
                    total = jnp.where(mask, value, total)
                for value in extra.get(n, ()):
                    total = total + value
                store(n, total)

        shift_bits = 22
        factor = (1 << shift_bits) // width + 1
        for c in range(chunks):
            index = lax.broadcasted_iota(jnp.int32, (1, CHUNK), 1) + c * CHUNK
            column = index - width * ((index * factor) >> shift_bits)
            nw_ref[:, pl.ds(c * CHUNK, CHUNK)] = jnp.where(column == 0, 0.0, 1.0)
            ne_ref[:, pl.ds(c * CHUNK, CHUNK)] = jnp.where(column == width - 1, 0.0, 1.0)
        tail = wide - LANES
        m_ref[:, :, :LANES] = jnp.zeros((slots * fields_n, levels, LANES), jnp.float32)
        m_ref[:, :, tail + LANES :] = jnp.zeros((slots * fields_n, levels, 2 * LANES), jnp.float32)
        uv_ref[:, :, :LANES] = jnp.zeros((2, slots, LANES), jnp.float32)
        uv_ref[:, :, tail + LANES :] = jnp.zeros((2, slots, 2 * LANES), jnp.float32)
        for ref in (s_ref, u_ref):
            ref[:, :LANES] = jnp.zeros((slots, LANES), jnp.float32)
            ref[:, wide + LANES :] = jnp.zeros((slots, LANES), jnp.float32)
        w_ref[:, tail:] = jnp.zeros((slots, LANES), jnp.float32)
        d_ref[:, tail:] = jnp.zeros((slots, LANES), jnp.float32)

        def per_level(read):
            level = lax.broadcasted_iota(jnp.int32, (levels, 1), 0)
            value = jnp.zeros((levels, 1), jnp.float32)
            for n in range(levels):
                value = jnp.where(level == n, read(n), value)
            return value

        thick_col = per_level(lambda n: thick[n])
        mix_col = per_level(lambda n: mixing[n])

        copies[0].wait()
        copies[1].wait()
        spans = [(c * CHUNK, min(CHUNK, cells - c * CHUNK)) for c in range(chunks)]
        for at, size in spans:
            w_ref[:, pl.ds(at, size)] = wbuf[:, pl.ds(at, size)].astype(jnp.float32)
            d_ref[:, pl.ds(at, size)] = dbuf[:, pl.ds(at, size)] + 4.0
        for k in range(slots):
            copies[2 + k].wait()
            for f in range(fields_n):
                for at, size in spans:
                    masked = fbuf[k, f, :, pl.ds(at, size)] * w_ref[k : k + 1, pl.ds(at, size)]
                    m_ref[k * fields_n + f, :, pl.ds(LANES + at, size)] = masked
                    if f < 2:
                        uv_ref[f, k : k + 1, pl.ds(LANES + at, size)] = jnp.sum(
                            masked * thick_col, axis=0, keepdims=True
                        )

        for f in range(2):
            for e, rim in enumerate(extract(lambda n: uv_ref[f, :, pl.ds(LANES * (n + 1), LANES)], slots)):
                for k in range(slots):
                    pack1[POS[e], k, f : f + 1, :] = rim[k : k + 1]

        pl.semaphore_wait(barrier, peers)
        sent1 = exchange(pack1, near1, send1, recv1)

        def slab_pack(kf, carry):
            rims = extract(lambda n: m_ref[kf, :, pl.ds(LANES * (n + 1), LANES)], levels)
            for e, rim in enumerate(rims):
                packb[POS[e], kf] = rim
            return carry

        lax.fori_loop(0, slots * fields_n, slab_pack, 0)
        sentb = exchange(packb, nearb, sendb, recvb)

        def entry(k, e):
            dt, ds, p, code = (links[0, 0, k, e, n] for n in range(4))
            source = place(dt, tiles) * n_s + place(ds, strips)
            return source, jnp.maximum(p, 0), p, code

        def choose(number, test, yes, no):
            return jnp.where(test(jnp.full(yes.shape, number, jnp.int32)), yes, no)

        def turn(code):
            a = jnp.where(code == 0, 1.0, jnp.where(code == 2, -1.0, 0.0))
            b = jnp.where(code == 1, 1.0, jnp.where(code == 3, -1.0, 0.0))
            return a, b

        def surface_rims(near):
            for e in range(4):
                for k in range(slots):
                    source, slot, p, code = entry(k, e)
                    rim = near[source, POS[e ^ 1], slot]
                    rim = choose(code, lambda x: x != 0, flip(rim), rim)
                    rim_ref[e, k : k + 1, :] = choose(p, lambda x: x >= 0, rim, jnp.zeros_like(rim))

        def put_edges():
            def store(n, value):
                eb_ref[:, pl.ds(n * LANES, LANES)] = value

            insert(rim_ref[0], rim_ref[1], rim_ref[2], rim_ref[3], store)

        inner = slice(LANES, LANES + CHUNK)

        for copy in sent1:
            copy.wait_recv()
        for e in range(4):
            for k in range(slots):
                source, slot, p, code = entry(k, e)
                pair = near1[source, POS[e ^ 1], slot]
                pair = choose(code, lambda x: x != 0, flip(pair), pair)
                pair = choose(p, lambda x: x >= 0, pair, jnp.zeros_like(pair))
                a, b = turn(code)
                if e < 2:
                    rim = a * pair[0:1] + b * pair[1:2]
                else:
                    rim = a * pair[1:2] - b * pair[0:1]
                rim_ref[e, k : k + 1, :] = rim if e in (1, 3) else -rim
        put_edges()
        for c in range(chunks):
            at = c * CHUNK
            span = pl.ds(at, CHUNK)
            u_win = uv_ref[0, :, pl.ds(at, CHUNK + 2 * LANES)]
            v_win = uv_ref[1, :, pl.ds(at, CHUNK + 2 * LANES)]
            flux = ne_ref[:, span] * roll(u_win, -1)[:, inner] - nw_ref[:, span] * roll(u_win, 1)[:, inner]
            flux = flux + (roll(v_win, -width)[:, inner] - roll(v_win, width)[:, inner]) + eb_ref[:, span]
            s_ref[:, pl.ds(LANES + at, CHUNK)] = w_ref[:, span] * (0.5 * flux)

        def send_surface(x_ref, pack, near, send_sem, recv_sem):
            for e, rim in enumerate(extract(lambda n: x_ref[:, pl.ds(LANES * (n + 1), LANES)], slots)):
                for k in range(slots):
                    pack[POS[e], k, :, :] = rim[k : k + 1]
            return exchange(pack, near, send_sem, recv_sem)

        def image(x_ref, at):
            span = pl.ds(at, CHUNK)
            win = x_ref[:, pl.ds(at, CHUNK + 2 * LANES)]
            near = ne_ref[:, span] * roll(win, -1)[:, inner] + nw_ref[:, span] * roll(win, 1)[:, inner]
            near = near + (roll(win, -width)[:, inner] + roll(win, width)[:, inner]) + eb_ref[:, span]
            return w_ref[:, span] * (d_ref[:, span] * win[:, inner] - near)

        def slab_slot(k):
            for e in range(4):
                source, slot, p, code = entry(k, e)
                a, b = turn(code)
                got = []
                for f in range(fields_n):
                    rim = nearb[source, POS[e ^ 1], slot * fields_n + f]
                    rim = choose(code, lambda x: x != 0, flip(rim), rim)
                    got.append(choose(p, lambda x: x >= 0, rim, jnp.zeros_like(rim)))
                rims_ref[e, 0] = a * got[0] + b * got[1]
                rims_ref[e, 1] = a * got[1] - b * got[0]
                for f in range(2, fields_n):
                    rims_ref[e, f] = got[f]

            def one(f, carry):
                def store(n, value):
                    ebs_ref[:, pl.ds(n * LANES, LANES)] = value

                insert(rims_ref[0, f], rims_ref[1, f], rims_ref[2, f], rims_ref[3, f], store)
                spread_col = per_level(lambda n: spread[f, n])
                for at, size in spans:
                    span = pl.ds(at, CHUNK)
                    win = m_ref[k * fields_n + f, :, pl.ds(at, CHUNK + 2 * LANES)]
                    mid = win[:, inner]
                    flat = ne_ref[:, span] * roll(win, -1)[:, inner] + nw_ref[:, span] * roll(win, 1)[:, inner]
                    flat = flat + (roll(win, -width)[:, inner] + roll(win, width)[:, inner]) + ebs_ref[:, span]
                    flat = flat - 4.0 * mid
                    above = jnp.concatenate([mid[1:], mid[-1:]], 0)
                    below = jnp.concatenate([mid[:1], mid[:-1]], 0)
                    column = above + below - 2.0 * mid
                    new = w_ref[k : k + 1, span] * (mid + spread_col * flat + mix_col * column)
                    fbuf[k, f, :, pl.ds(at, size)] = new[:, :size]
                return carry

            lax.fori_loop(0, fields_n, one, 0)
            copy = pltpu.make_async_copy(fbuf.at[k], out_f.at[0, 0, k], out_sem.at[k])
            copy.start()
            return copy

        def slab_part(part):
            return [slab_slot(k) for k in range(slots) if k * 3 // slots == part]

        sent2 = send_surface(s_ref, pack2, near2, send2, recv2)
        for copy in sentb:
            copy.wait_recv()
        put_out = slab_part(0)
        for copy in sent2:
            copy.wait_recv()
        surface_rims(near2)
        put_edges()
        for c in range(chunks):
            u_ref[:, pl.ds(LANES + c * CHUNK, CHUNK)] = image(s_ref, c * CHUNK)
        sent3 = send_surface(u_ref, pack3, near3, send3, recv3)
        put_out += slab_part(1)
        for copy in sent3:
            copy.wait_recv()
        surface_rims(near3)
        put_edges()
        blank = jnp.zeros((slots, CHUNK), jnp.float32)

        def whole(value):
            return jnp.sum(jnp.sum(value, axis=1, keepdims=True), axis=0, keepdims=True)

        ss = su = uu = uv = blank
        for c in range(chunks):
            x = s_ref[:, pl.ds(LANES + c * CHUNK, CHUNK)]
            y = u_ref[:, pl.ds(LANES + c * CHUNK, CHUNK)]
            z = image(u_ref, c * CHUNK)
            v_ref[:, pl.ds(c * CHUNK, CHUNK)] = z
            ss, su, uu, uv = ss + x * x, su + x * y, uu + y * y, uv + y * z
        ss, su, uu, uv = whole(ss), whole(su), whole(uu), whole(uv)
        ratio = jnp.where(su > 0.0, ss / su, 0.0)
        ee = eu = ef = uf = blank
        for c in range(chunks):
            x = s_ref[:, pl.ds(LANES + c * CHUNK, CHUNK)]
            y = u_ref[:, pl.ds(LANES + c * CHUNK, CHUNK)]
            z = v_ref[:, pl.ds(c * CHUNK, CHUNK)]
            left = x - ratio * y
            left_image = y - ratio * z
            ee, eu, ef = ee + left * left, eu + left * y, ef + left * left_image
            uf = uf + (y * left_image + left * z)
        row = jnp.zeros((1, LANES), jnp.float32)
        for n, value in enumerate((ss, su, ratio, whole(ee), whole(eu), uu, whole(ef), whole(uf), uv)):
            row = jnp.where(lane == n, value, row)
        row_ref[...] = row
        red_ref[me_first] = row

        def first_copy(j):
            other = lax.rem(me_first + j, first)
            return pltpu.make_async_remote_copy(
                src_ref=row_ref,
                dst_ref=red_ref.at[me_first],
                send_sem=sendr.at[j],
                recv_sem=recvr.at[me_first],
                device_id=(base + other // strips, other % strips),
                device_id_type=pl.DeviceIdType.MESH,
            )

        def first_arrival(j):
            other = lax.rem(me_first + j, first)
            return pltpu.make_async_remote_copy(
                src_ref=row_ref,
                dst_ref=red_ref.at[other],
                send_sem=sendr.at[j],
                recv_sem=recvr.at[other],
                device_id=(base + other // strips, other % strips),
                device_id_type=pl.DeviceIdType.MESH,
            )

        for j in range(1, first):
            first_copy(j).start()
        put_out += slab_part(2)
        for j in range(1, first):
            first_arrival(j).wait_recv()

        if high > 1:
            mine = t // low
            copies2 = []
            for j in range(1, high):
                other = lax.rem(mine + j, high)
                copy = pltpu.make_async_remote_copy(
                    src_ref=red_ref,
                    dst_ref=red2_ref.at[mine],
                    send_sem=sendq.at[j],
                    recv_sem=recvq.at[mine],
                    device_id=(other * low + place_t, s),
                    device_id_type=pl.DeviceIdType.MESH,
                )
                copy.start()
                copies2.append(copy)
            red2_ref[mine] = red_ref[...]
            for j in range(1, high):
                other = lax.rem(mine + j, high)
                pltpu.make_async_remote_copy(
                    src_ref=red_ref,
                    dst_ref=red2_ref.at[other],
                    send_sem=sendq.at[j],
                    recv_sem=recvq.at[other],
                    device_id=(other * low + place_t, s),
                    device_id_type=pl.DeviceIdType.MESH,
                ).wait_recv()
            for copy in copies2:
                copy.wait_send()
            rows = [red2_ref[n] for n in range(high)]
        else:
            rows = [red_ref[...]]

        total = sum(jnp.sum(x, axis=0) for x in rows)
        rr0, sas = total[:, 0:1], total[:, 1:2]
        alpha0 = rr0 / sas
        moved = jnp.zeros((1, LANES), jnp.float32)
        lane3 = lax.broadcasted_iota(jnp.int32, (1, 1, LANES), 2)
        for x in rows:
            delta = jnp.broadcast_to(x[:, :, 2:3], x.shape) - alpha0[None]
            weight = jnp.where(
                (lane3 == 3) | (lane3 == 6), 1.0,
                jnp.where(lane3 == 4, 2.0 * delta, jnp.where(lane3 == 7, delta, delta * delta)),
            )
            moved = moved + jnp.sum(x * weight, axis=0)
        rr1 = jnp.sum(jnp.where((lane >= 3) & (lane <= 5), moved, 0.0), axis=1, keepdims=True)
        rar = jnp.sum(jnp.where((lane >= 6) & (lane <= 8), moved, 0.0), axis=1, keepdims=True)
        beta = rr1 / rr0
        alpha1 = rr1 / (rar - beta * rr1 / alpha0)
        for at, size in spans:
            x = s_ref[:, pl.ds(LANES + at, CHUNK)]
            y = u_ref[:, pl.ds(LANES + at, CHUNK)]
            z = v_ref[:, pl.ds(at, CHUNK)]
            r1 = x - alpha0 * y
            direction = r1 + beta * x
            direction_image = (y - alpha0 * z) + beta * y
            out_x[0, 0, :, pl.ds(at, size)] = (alpha0 * x + alpha1 * direction)[:, :size]
            out_r[0, 0, :, pl.ds(at, size)] = (r1 - alpha1 * direction_image)[:, :size]

        for copy in sent1 + sentb + sent2 + sent3:
            copy.wait_send()
        for j in range(1, first):
            first_copy(j).wait_send()
        for copy in put_out:
            copy.wait()

    f32 = jnp.float32
    any_space = pl.BlockSpec(memory_space=pl.ANY)
    smem = pl.BlockSpec(memory_space=pltpu.SMEM)
    vmem = pl.BlockSpec(memory_space=pltpu.VMEM)
    kf = slots * fields_n
    dma = pltpu.SemaphoreType.DMA
    return pl.pallas_call(
        kernel,
        out_shape=(
            jax.ShapeDtypeStruct((1, 1, slots, fields_n, levels, cells), f32),
            jax.ShapeDtypeStruct((1, 1, slots, cells), f32),
            jax.ShapeDtypeStruct((1, 1, slots, cells), f32),
        ),
        in_specs=[any_space, any_space, smem, any_space, smem, smem, smem],
        out_specs=(any_space, vmem, vmem),
        scratch_shapes=[
            pltpu.VMEM((slots, fields_n, levels, cells), f32),
            pltpu.VMEM((slots, cells), jnp.int32),
            pltpu.VMEM((slots, cells), f32),
            pltpu.VMEM((kf, levels, padded), f32),
            pltpu.VMEM((slots, wide), f32),
            pltpu.VMEM((slots, wide), f32),
            pltpu.VMEM((1, wide), f32),
            pltpu.VMEM((1, wide), f32),
            pltpu.VMEM((2, slots, padded), f32),
            pltpu.VMEM((slots, padded), f32),
            pltpu.VMEM((slots, padded), f32),
            pltpu.VMEM((slots, wide), f32),
            pltpu.VMEM((slots, wide), f32),
            pltpu.VMEM((levels, wide), f32),
            pltpu.VMEM((4, slots, LANES), f32),
            pltpu.VMEM((4, fields_n, levels, LANES), f32),
            pltpu.VMEM((4, slots, 2, LANES), f32),
            pltpu.VMEM((n_dirs, 4, slots, 2, LANES), f32),
            pltpu.VMEM((4, kf, levels, LANES), f32),
            pltpu.VMEM((n_dirs, 4, kf, levels, LANES), f32),
            pltpu.VMEM((4, slots, 1, LANES), f32),
            pltpu.VMEM((n_dirs, 4, slots, 1, LANES), f32),
            pltpu.VMEM((4, slots, 1, LANES), f32),
            pltpu.VMEM((n_dirs, 4, slots, 1, LANES), f32),
            pltpu.VMEM((1, LANES), f32),
            pltpu.VMEM((first, 1, LANES), f32),
            pltpu.VMEM((high, first, 1, LANES) if high > 1 else (1, 1, 1, LANES), f32),
            dma((2 + slots,)),
            dma((slots,)),
            dma((n_dirs,)), dma((n_dirs,)), dma((n_dirs,)), dma((n_dirs,)),
            dma((n_dirs,)), dma((n_dirs,)), dma((n_dirs,)), dma((n_dirs,)),
            dma((first,)), dma((first,)), dma((high,)), dma((high,)),
        ],
        compiler_params=pltpu.CompilerParams(collective_id=0, has_side_effects=True),
    )


def solution(mesh):
    tiles, strips = mesh.shape["tiles"], mesh.shape["strip"]

    def on_device(fields, wet_land, links, surface_diagonal, spread, mixing, thickness):
        slots, fields_n, levels, cells = fields.shape[2:]
        call = build(tiles, strips, slots, fields_n, levels, cells)
        return call(fields, wet_land, links, surface_diagonal, spread, mixing, thickness)

    placed = (
        P("tiles", "strip", None, None, None, None),
        P("tiles", "strip", None, None),
        P("tiles", "strip", None, None, None),
        P("tiles", "strip", None, None),
        P(),
        P(),
        P(),
    )
    return jax.shard_map(
        on_device,
        mesh=mesh,
        in_specs=placed,
        out_specs=(
            P("tiles", "strip", None, None, None, None),
            P("tiles", "strip", None, None),
            P("tiles", "strip", None, None),
        ),
        check_vma=False,
    )
```

```python
import math

import jax
import jax.numpy as jnp
from jax import lax
from jax.experimental import pallas as pl
from jax.experimental.pallas import tpu as pltpu
from jax.sharding import PartitionSpec as P

LANES = 128
CHUNK = 1024
POS = (0, 3, 1, 2)
GROUP = 16


def offsets(size):
    return (-1, 0, 1) if size >= 3 else tuple(range(size))


def place(offset, size):
    if size >= 3:
        return offset + 1
    return offset * offset if size == 2 else 0 * offset


def roll(value, shift, axis=1):
    size = value.shape[axis]
    shift = shift % size
    return pltpu.roll(value, shift, axis) if shift else value


def build(tiles, strips, slots, fields_n, levels, cells):
    width = math.isqrt(cells)
    n_tiles = -(-cells // CHUNK) * CHUNK // LANES
    wide = n_tiles * LANES
    padded = wide + 2 * LANES
    chunks = wide // CHUNK
    steps_t, steps_s = offsets(tiles), offsets(strips)
    n_s = len(steps_s)
    n_dirs = len(steps_t) * n_s
    low = min(GROUP, tiles)
    high = tiles // low
    first = low * strips
    directions = []
    for dt in steps_t:
        for ds in steps_s:
            if dt == 0 and ds == 0:
                continue
            sides = []
            if dt == -1 or (tiles == 2 and dt):
                sides.append(0)
            if ds == -1 or (strips == 2 and ds):
                sides.append(1)
            if ds == 1:
                sides.append(2)
            if dt == 1:
                sides.append(3)
            here = place(dt, tiles) * n_s + place(ds, strips)
            back = place(-dt if tiles >= 3 else dt, tiles) * n_s + place(-ds if strips >= 3 else ds, strips)
            directions.append((dt, ds, here, back, min(sides), max(sides) + 1))

    def kernel(
        fields, wet_in, links_in, diag_in, spread_in, mixing_in, thick_in, out_f, out_x, out_r,
        links, spread, mixing, thick, fbuf, wbuf, dbuf, m_ref, w_ref, d_ref, nw_ref, ne_ref, uv_ref, s_ref, u_ref, v_ref, eb_ref, ebs_ref,
        rim_ref, rims_ref, pack1, near1, packb, nearb, pack2, near2, pack3, near3, row_ref, red_ref, red2_ref,
        in_sem, send1, recv1, sendb, recvb, send2, recv2, send3, recv3, sendr, recvr, sendq, recvq,
    ):
        t = lax.axis_index("tiles")
        s = lax.axis_index("strip")
        copies = [
            pltpu.make_async_copy(wet_in.at[0], wbuf, in_sem.at[0]),
            pltpu.make_async_copy(diag_in.at[0], dbuf, in_sem.at[1]),
        ] + [pltpu.make_async_copy(fields.at[0, 0, k], fbuf.at[k], in_sem.at[2 + k]) for k in range(slots)]
        small = [
            pltpu.make_async_copy(thick_in, thick, in_sem.at[2 + slots]),
            pltpu.make_async_copy(mixing_in, mixing, in_sem.at[3 + slots]),
            pltpu.make_async_copy(spread_in, spread, in_sem.at[4 + slots]),
            pltpu.make_async_copy(links_in.at[0, 0], links, in_sem.at[5 + slots]),
        ]
        for copy in copies[:3] + small + copies[3:]:
            copy.start()

        barrier = pltpu.get_barrier_semaphore()
        base = (t // low) * low
        place_t = t % low
        me_first = place_t * strips + s
        peers = 0
        for j in range(1, first):
            other = lax.rem(me_first + j, first)
            pl.semaphore_signal(
                barrier, inc=1, device_id=(base + other // strips, other % strips),
                device_id_type=pl.DeviceIdType.MESH,
            )
            peers += 1
        for j in range(1, high):
            other = lax.rem(t // low + j, high)
            pl.semaphore_signal(
                barrier, inc=1, device_id=(other * low + place_t, s), device_id_type=pl.DeviceIdType.MESH
            )
            peers += 1
        if high > 1:
            for dt, ds, here, back, lo, hi in directions:
                pl.semaphore_signal(
                    barrier, inc=1,
                    device_id=(lax.rem(t + dt + tiles, tiles), lax.rem(s + ds + strips, strips)),
                    device_id_type=pl.DeviceIdType.MESH,
                )
                peers += 1

        def exchange(pack, near, send_sem, recv_sem):
            out = []
            for dt, ds, here, back, lo, hi in directions:
                copy = pltpu.make_async_remote_copy(
                    src_ref=pack.at[pl.ds(lo, hi - lo)],
                    dst_ref=near.at[back, pl.ds(lo, hi - lo)],
                    send_sem=send_sem.at[here],
                    recv_sem=recv_sem.at[back],
                    device_id=(lax.rem(t + dt + tiles, tiles), lax.rem(s + ds + strips, strips)),
                    device_id_type=pl.DeviceIdType.MESH,
                )
                copy.start()
                out.append(copy)
            return out

        lane = lax.broadcasted_iota(jnp.int32, (1, LANES), 1)
        flip_at = jnp.where(lane < width, width - 1 - lane, lane)

        def flip(value):
            rows = value.shape[0]
            if rows < 8:
                value = jnp.concatenate([value, jnp.zeros((8 - rows, LANES), jnp.float32)], 0)
            at = jnp.broadcast_to(flip_at, value.shape)
            return jnp.take_along_axis(value, at, axis=1)[:rows]

        def extract(tile, rows):
            blank = jnp.zeros((rows, LANES), jnp.float32)
            parts_w, parts_e = [blank] * 4, [blank] * 4
            loaded = {}

            def at(n):
                if n not in loaded:
                    loaded[n] = tile(n)
                return loaded[n]

            for i in range(-1, width):
                pe = width * i + width - 1
                pw = pe + 1
                shift = (i - pe) % LANES
                turned = {}
                for n in {pe // LANES if i >= 0 else pw // LANES, pw // LANES if i + 1 < width else pe // LANES}:
                    turned[n] = roll(at(n), shift)
                if i >= 0:
                    parts_e[i % 4] = jnp.where(lane == i, turned[pe // LANES], parts_e[i % 4])
                if i + 1 < width:
                    parts_w[i % 4] = jnp.where(lane == i + 1, turned[pw // LANES], parts_w[i % 4])
            west = (parts_w[0] + parts_w[1]) + (parts_w[2] + parts_w[3])
            east = (parts_e[0] + parts_e[1]) + (parts_e[2] + parts_e[3])

            def line(start):
                a, n = start % LANES, start // LANES
                if a == 0:
                    return jnp.where(lane < width, at(n), 0.0)
                head = roll(at(n), -a)
                if a + width <= LANES:
                    return jnp.where(lane < width, head, 0.0)
                tail = roll(at(n + 1), -a)
                return jnp.where(lane < LANES - a, head, jnp.where(lane < width, tail, 0.0))

            return west, east, line(0), line(width * (width - 1))

        def insert(west, east, south, north, store):
            even = (lane & 1) == 0
            mixed = (jnp.where(even, east, west), jnp.where(even, west, east))
            tiles_of = {}

            def add(n, mask, value):
                tiles_of.setdefault(n, []).append((mask, value))

            for i in range(-1, width):
                pe = width * i + width - 1
                pw = pe + 1
                turned = roll(mixed[i % 2], (pe - i) % LANES)
                if i >= 0 and i + 1 < width and pe // LANES == pw // LANES:
                    mask = (lane == pe % LANES) | (lane == pw % LANES)
                    add(pe // LANES, mask, turned)
                else:
                    if i >= 0:
                        add(pe // LANES, lane == pe % LANES, turned)
                    if i + 1 < width:
                        add(pw // LANES, lane == pw % LANES, turned)
            extra = {}
            for start, rim in ((0, south), (width * (width - 1), north)):
                a, n = start % LANES, start // LANES
                turned = roll(rim, a)
                extra.setdefault(n, []).append(jnp.where(lane >= a, turned, 0.0) if a else turned)
                if a + width > LANES:
                    extra.setdefault(n + 1, []).append(jnp.where(lane < a + width - LANES, turned, 0.0))
            blank = jnp.zeros(west.shape, jnp.float32)
            for n in range(n_tiles):
                total = blank
                for mask, value in tiles_of.get(n, ()):
                    total = jnp.where(mask, value, total)
                for value in extra.get(n, ()):
                    total = total + value
                store(n, total)

        shift_bits = 22
        factor = (1 << shift_bits) // width + 1
        for c in range(chunks):
            index = lax.broadcasted_iota(jnp.int32, (1, CHUNK), 1) + c * CHUNK
            column = index - width * ((index * factor) >> shift_bits)
            nw_ref[:, pl.ds(c * CHUNK, CHUNK)] = jnp.where(column == 0, 0.0, 1.0)
            ne_ref[:, pl.ds(c * CHUNK, CHUNK)] = jnp.where(column == width - 1, 0.0, 1.0)
        tail = wide - LANES
        m_ref[:, :, :LANES] = jnp.zeros((slots * fields_n, levels, LANES), jnp.float32)
        m_ref[:, :, tail + LANES :] = jnp.zeros((slots * fields_n, levels, 2 * LANES), jnp.float32)
        uv_ref[:, :, :LANES] = jnp.zeros((2, slots, LANES), jnp.float32)
        uv_ref[:, :, tail + LANES :] = jnp.zeros((2, slots, 2 * LANES), jnp.float32)
        for ref in (s_ref, u_ref):
            ref[:, :LANES] = jnp.zeros((slots, LANES), jnp.float32)
            ref[:, wide + LANES :] = jnp.zeros((slots, LANES), jnp.float32)
        w_ref[:, tail:] = jnp.zeros((slots, LANES), jnp.float32)
        d_ref[:, tail:] = jnp.zeros((slots, LANES), jnp.float32)

        def per_level(read):
            level = lax.broadcasted_iota(jnp.int32, (levels, 1), 0)
            value = jnp.zeros((levels, 1), jnp.float32)
            for n in range(levels):
                value = jnp.where(level == n, read(n), value)
            return value

        for copy in small:
            copy.wait()
        thick_col = per_level(lambda n: thick[n])
        mix_col = per_level(lambda n: mixing[n])

        copies[0].wait()
        copies[1].wait()
        spans = [(c * CHUNK, min(CHUNK, cells - c * CHUNK)) for c in range(chunks)]
        for k in range(slots):
            for at, size in spans:
                w_ref[k : k + 1, pl.ds(at, size)] = wbuf[k, :, pl.ds(at, size)].astype(jnp.float32)
                d_ref[k : k + 1, pl.ds(at, size)] = dbuf[k, :, pl.ds(at, size)] + 4.0
        for k in range(slots):
            copies[2 + k].wait()
            for f in range(fields_n):
                for at, size in spans:
                    masked = fbuf[k, f, :, pl.ds(at, size)] * w_ref[k : k + 1, pl.ds(at, size)]
                    m_ref[k * fields_n + f, :, pl.ds(LANES + at, size)] = masked
                    if f < 2:
                        uv_ref[f, k : k + 1, pl.ds(LANES + at, size)] = jnp.sum(
                            masked * thick_col, axis=0, keepdims=True
                        )

        for f in range(2):
            for e, rim in enumerate(extract(lambda n: uv_ref[f, :, pl.ds(LANES * (n + 1), LANES)], slots)):
                for k in range(slots):
                    pack1[POS[e], k, f : f + 1, :] = rim[k : k + 1]

        pl.semaphore_wait(barrier, peers)
        sent1 = exchange(pack1, near1, send1, recv1)

        def slab_pack(kf, carry):
            rims = extract(lambda n: m_ref[kf, :, pl.ds(LANES * (n + 1), LANES)], levels)
            for e, rim in enumerate(rims):
                packb[POS[e], kf] = rim
            return carry

        lax.fori_loop(0, slots * fields_n, slab_pack, 0)
        sentb = exchange(packb, nearb, sendb, recvb)

        def entry(k, e):
            dt, ds, p, code = (links[k, e, n] for n in range(4))
            source = place(dt, tiles) * n_s + place(ds, strips)
            return source, jnp.maximum(p, 0), p, code

        def choose(number, test, yes, no):
            return jnp.where(test(jnp.full(yes.shape, number, jnp.int32)), yes, no)

        def turn(code):
            a = jnp.where(code == 0, 1.0, jnp.where(code == 2, -1.0, 0.0))
            b = jnp.where(code == 1, 1.0, jnp.where(code == 3, -1.0, 0.0))
            return a, b

        def surface_rims(near):
            for e in range(4):
                for k in range(slots):
                    source, slot, p, code = entry(k, e)
                    rim = near[source, POS[e ^ 1], slot]
                    rim = choose(code, lambda x: x != 0, flip(rim), rim)
                    rim_ref[e, k : k + 1, :] = choose(p, lambda x: x >= 0, rim, jnp.zeros_like(rim))

        def put_edges():
            def store(n, value):
                eb_ref[:, pl.ds(n * LANES, LANES)] = value

            insert(rim_ref[0], rim_ref[1], rim_ref[2], rim_ref[3], store)

        inner = slice(LANES, LANES + CHUNK)

        for copy in sent1:
            copy.wait_recv()
        for e in range(4):
            for k in range(slots):
                source, slot, p, code = entry(k, e)
                pair = near1[source, POS[e ^ 1], slot]
                pair = choose(code, lambda x: x != 0, flip(pair), pair)
                pair = choose(p, lambda x: x >= 0, pair, jnp.zeros_like(pair))
                a, b = turn(code)
                if e < 2:
                    rim = a * pair[0:1] + b * pair[1:2]
                else:
                    rim = a * pair[1:2] - b * pair[0:1]
                rim_ref[e, k : k + 1, :] = rim if e in (1, 3) else -rim
        put_edges()
        for c in range(chunks):
            at = c * CHUNK
            span = pl.ds(at, CHUNK)
            u_win = uv_ref[0, :, pl.ds(at, CHUNK + 2 * LANES)]
            v_win = uv_ref[1, :, pl.ds(at, CHUNK + 2 * LANES)]
            flux = ne_ref[:, span] * roll(u_win, -1)[:, inner] - nw_ref[:, span] * roll(u_win, 1)[:, inner]
            flux = flux + (roll(v_win, -width)[:, inner] - roll(v_win, width)[:, inner]) + eb_ref[:, span]
            s_ref[:, pl.ds(LANES + at, CHUNK)] = w_ref[:, span] * (0.5 * flux)

        def send_surface(x_ref, pack, near, send_sem, recv_sem):
            for e, rim in enumerate(extract(lambda n: x_ref[:, pl.ds(LANES * (n + 1), LANES)], slots)):
                for k in range(slots):
                    pack[POS[e], k, :, :] = rim[k : k + 1]
            return exchange(pack, near, send_sem, recv_sem)

        def image(x_ref, at):
            span = pl.ds(at, CHUNK)
            win = x_ref[:, pl.ds(at, CHUNK + 2 * LANES)]
            near = ne_ref[:, span] * roll(win, -1)[:, inner] + nw_ref[:, span] * roll(win, 1)[:, inner]
            near = near + (roll(win, -width)[:, inner] + roll(win, width)[:, inner]) + eb_ref[:, span]
            return w_ref[:, span] * (d_ref[:, span] * win[:, inner] - near)

        def slab_slot(k):
            for e in range(4):
                source, slot, p, code = entry(k, e)
                a, b = turn(code)
                got = []
                for f in range(fields_n):
                    rim = nearb[source, POS[e ^ 1], slot * fields_n + f]
                    rim = choose(code, lambda x: x != 0, flip(rim), rim)
                    got.append(choose(p, lambda x: x >= 0, rim, jnp.zeros_like(rim)))
                rims_ref[e, 0] = a * got[0] + b * got[1]
                rims_ref[e, 1] = a * got[1] - b * got[0]
                for f in range(2, fields_n):
                    rims_ref[e, f] = got[f]

            def one(f, carry):
                def store(n, value):
                    ebs_ref[:, pl.ds(n * LANES, LANES)] = value

                insert(rims_ref[0, f], rims_ref[1, f], rims_ref[2, f], rims_ref[3, f], store)
                spread_col = per_level(lambda n: spread[f, n])
                for at, size in spans:
                    span = pl.ds(at, CHUNK)
                    win = m_ref[k * fields_n + f, :, pl.ds(at, CHUNK + 2 * LANES)]
                    mid = win[:, inner]
                    flat = ne_ref[:, span] * roll(win, -1)[:, inner] + nw_ref[:, span] * roll(win, 1)[:, inner]
                    flat = flat + (roll(win, -width)[:, inner] + roll(win, width)[:, inner]) + ebs_ref[:, span]
                    flat = flat - 4.0 * mid
                    above = jnp.concatenate([mid[1:], mid[-1:]], 0)
                    below = jnp.concatenate([mid[:1], mid[:-1]], 0)
                    column = above + below - 2.0 * mid
                    new = w_ref[k : k + 1, span] * (mid + spread_col * flat + mix_col * column)
                    out_f[0, 0, k, f, :, pl.ds(at, size)] = new[:, :size]
                return carry

            lax.fori_loop(0, fields_n, one, 0)

        def slab_part(part):
            for k in range(slots):
                if k * 3 // slots == part:
                    slab_slot(k)

        sent2 = send_surface(s_ref, pack2, near2, send2, recv2)
        for copy in sentb:
            copy.wait_recv()
        slab_part(0)
        for copy in sent2:
            copy.wait_recv()
        surface_rims(near2)
        put_edges()
        for c in range(chunks):
            u_ref[:, pl.ds(LANES + c * CHUNK, CHUNK)] = image(s_ref, c * CHUNK)
        sent3 = send_surface(u_ref, pack3, near3, send3, recv3)
        slab_part(1)
        for copy in sent3:
            copy.wait_recv()
        surface_rims(near3)
        put_edges()
        blank = jnp.zeros((slots, CHUNK), jnp.float32)

        def whole(value):
            return jnp.sum(jnp.sum(value, axis=1, keepdims=True), axis=0, keepdims=True)

        ss = su = uu = uv = blank
        for c in range(chunks):
            x = s_ref[:, pl.ds(LANES + c * CHUNK, CHUNK)]
            y = u_ref[:, pl.ds(LANES + c * CHUNK, CHUNK)]
            z = image(u_ref, c * CHUNK)
            v_ref[:, pl.ds(c * CHUNK, CHUNK)] = z
            ss, su, uu, uv = ss + x * x, su + x * y, uu + y * y, uv + y * z
        ss, su, uu, uv = whole(ss), whole(su), whole(uu), whole(uv)
        ratio = jnp.where(su > 0.0, ss / su, 0.0)
        ee = eu = ef = uf = blank
        for c in range(chunks):
            x = s_ref[:, pl.ds(LANES + c * CHUNK, CHUNK)]
            y = u_ref[:, pl.ds(LANES + c * CHUNK, CHUNK)]
            z = v_ref[:, pl.ds(c * CHUNK, CHUNK)]
            left = x - ratio * y
            left_image = y - ratio * z
            ee, eu, ef = ee + left * left, eu + left * y, ef + left * left_image
            uf = uf + (y * left_image + left * z)
        row = jnp.zeros((1, LANES), jnp.float32)
        for n, value in enumerate((ss, su, ratio, whole(ee), whole(eu), uu, whole(ef), whole(uf), uv)):
            row = jnp.where(lane == n, value, row)
        row_ref[...] = row
        red_ref[me_first] = row

        def first_copy(j):
            other = lax.rem(me_first + j, first)
            return pltpu.make_async_remote_copy(
                src_ref=row_ref,
                dst_ref=red_ref.at[me_first],
                send_sem=sendr.at[j],
                recv_sem=recvr.at[me_first],
                device_id=(base + other // strips, other % strips),
                device_id_type=pl.DeviceIdType.MESH,
            )

        def first_arrival(j):
            other = lax.rem(me_first + j, first)
            return pltpu.make_async_remote_copy(
                src_ref=row_ref,
                dst_ref=red_ref.at[other],
                send_sem=sendr.at[j],
                recv_sem=recvr.at[other],
                device_id=(base + other // strips, other % strips),
                device_id_type=pl.DeviceIdType.MESH,
            )

        for j in range(1, first):
            first_copy(j).start()
        slab_part(2)
        for j in range(1, first):
            first_arrival(j).wait_recv()

        if high > 1:
            mine = t // low
            copies2 = []
            for j in range(1, high):
                other = lax.rem(mine + j, high)
                copy = pltpu.make_async_remote_copy(
                    src_ref=red_ref,
                    dst_ref=red2_ref.at[mine],
                    send_sem=sendq.at[j],
                    recv_sem=recvq.at[mine],
                    device_id=(other * low + place_t, s),
                    device_id_type=pl.DeviceIdType.MESH,
                )
                copy.start()
                copies2.append(copy)
            red2_ref[mine] = red_ref[...]
            for j in range(1, high):
                other = lax.rem(mine + j, high)
                pltpu.make_async_remote_copy(
                    src_ref=red_ref,
                    dst_ref=red2_ref.at[other],
                    send_sem=sendq.at[j],
                    recv_sem=recvq.at[other],
                    device_id=(other * low + place_t, s),
                    device_id_type=pl.DeviceIdType.MESH,
                ).wait_recv()
            for copy in copies2:
                copy.wait_send()
            rows = [red2_ref[n] for n in range(high)]
        else:
            rows = [red_ref[...]]

        total = sum(jnp.sum(x, axis=0) for x in rows)
        rr0, sas = total[:, 0:1], total[:, 1:2]
        alpha0 = rr0 / sas
        moved = jnp.zeros((1, LANES), jnp.float32)
        lane3 = lax.broadcasted_iota(jnp.int32, (1, 1, LANES), 2)
        for x in rows:
            delta = jnp.broadcast_to(x[:, :, 2:3], x.shape) - alpha0[None]
            weight = jnp.where(
                (lane3 == 3) | (lane3 == 6), 1.0,
                jnp.where(lane3 == 4, 2.0 * delta, jnp.where(lane3 == 7, delta, delta * delta)),
            )
            moved = moved + jnp.sum(x * weight, axis=0)
        rr1 = jnp.sum(jnp.where((lane >= 3) & (lane <= 5), moved, 0.0), axis=1, keepdims=True)
        rar = jnp.sum(jnp.where((lane >= 6) & (lane <= 8), moved, 0.0), axis=1, keepdims=True)
        beta = rr1 / rr0
        alpha1 = rr1 / (rar - beta * rr1 / alpha0)
        for at, size in spans:
            x = s_ref[:, pl.ds(LANES + at, CHUNK)]
            y = u_ref[:, pl.ds(LANES + at, CHUNK)]
            z = v_ref[:, pl.ds(at, CHUNK)]
            r1 = x - alpha0 * y
            direction = r1 + beta * x
            direction_image = (y - alpha0 * z) + beta * y
            answer = alpha0 * x + alpha1 * direction
            left = r1 - alpha1 * direction_image
            for k in range(slots):
                out_x[0, k, :, pl.ds(at, size)] = answer[k : k + 1, :size]
                out_r[0, k, :, pl.ds(at, size)] = left[k : k + 1, :size]

        for copy in sent1 + sentb + sent2 + sent3:
            copy.wait_send()
        for j in range(1, first):
            first_copy(j).wait_send()

    f32 = jnp.float32
    any_space = pl.BlockSpec(memory_space=pl.ANY)
    hbm = pl.BlockSpec(memory_space=pltpu.HBM)
    vmem = pl.BlockSpec(memory_space=pltpu.VMEM)
    kf = slots * fields_n
    dma = pltpu.SemaphoreType.DMA
    return pl.pallas_call(
        kernel,
        out_shape=(
            pltpu.VMEM((1, 1, slots, fields_n, levels, cells), f32),
            pltpu.VMEM((1, slots, 1, cells), f32),
            pltpu.VMEM((1, slots, 1, cells), f32),
        ),
        in_specs=[hbm] * 7,
        out_specs=(vmem, vmem, vmem),
        scratch_shapes=[
            pltpu.SMEM((slots, 4, 4), jnp.int32),
            pltpu.SMEM((fields_n, levels), f32),
            pltpu.SMEM((levels,), f32),
            pltpu.SMEM((levels,), f32),
            pltpu.VMEM((slots, fields_n, levels, cells), f32),
            pltpu.VMEM((slots, 1, cells), jnp.int32),
            pltpu.VMEM((slots, 1, cells), f32),
            pltpu.VMEM((kf, levels, padded), f32),
            pltpu.VMEM((slots, wide), f32),
            pltpu.VMEM((slots, wide), f32),
            pltpu.VMEM((1, wide), f32),
            pltpu.VMEM((1, wide), f32),
            pltpu.VMEM((2, slots, padded), f32),
            pltpu.VMEM((slots, padded), f32),
            pltpu.VMEM((slots, padded), f32),
            pltpu.VMEM((slots, wide), f32),
            pltpu.VMEM((slots, wide), f32),
            pltpu.VMEM((levels, wide), f32),
            pltpu.VMEM((4, slots, LANES), f32),
            pltpu.VMEM((4, fields_n, levels, LANES), f32),
            pltpu.VMEM((4, slots, 2, LANES), f32),
            pltpu.VMEM((n_dirs, 4, slots, 2, LANES), f32),
            pltpu.VMEM((4, kf, levels, LANES), f32),
            pltpu.VMEM((n_dirs, 4, kf, levels, LANES), f32),
            pltpu.VMEM((4, slots, 1, LANES), f32),
            pltpu.VMEM((n_dirs, 4, slots, 1, LANES), f32),
            pltpu.VMEM((4, slots, 1, LANES), f32),
            pltpu.VMEM((n_dirs, 4, slots, 1, LANES), f32),
            pltpu.VMEM((1, LANES), f32),
            pltpu.VMEM((first, 1, LANES), f32),
            pltpu.VMEM((high, first, 1, LANES) if high > 1 else (1, 1, 1, LANES), f32),
            dma((6 + slots,)),
            dma((n_dirs,)), dma((n_dirs,)), dma((n_dirs,)), dma((n_dirs,)),
            dma((n_dirs,)), dma((n_dirs,)), dma((n_dirs,)), dma((n_dirs,)),
            dma((first,)), dma((first,)), dma((high,)), dma((high,)),
        ],
        compiler_params=pltpu.CompilerParams(
            collective_id=0, has_side_effects=True, vmem_limit_bytes=58 << 20
        ),
    )


def put(*arrays):
    def kernel(*refs):
        count = len(arrays)
        sems = refs[-1]
        copies = [pltpu.make_async_copy(refs[n], refs[count + n], sems.at[n]) for n in range(count)]
        for copy in copies:
            copy.start()
        for copy in copies:
            copy.wait()

    return pl.pallas_call(
        kernel,
        out_shape=tuple(jax.ShapeDtypeStruct(x.shape, x.dtype) for x in arrays),
        in_specs=[pl.BlockSpec(memory_space=pl.ANY)] * len(arrays),
        out_specs=tuple(pl.BlockSpec(memory_space=pltpu.HBM) for _ in arrays),
        scratch_shapes=[pltpu.SemaphoreType.DMA((len(arrays),))],
        compiler_params=pltpu.CompilerParams(vmem_limit_bytes=1 << 20),
    )(*arrays)


def solution(mesh):
    tiles, strips = mesh.shape["tiles"], mesh.shape["strip"]

    def on_device(fields, wet_land, links, surface_diagonal, spread, mixing, thickness):
        slots, fields_n, levels, cells = fields.shape[2:]
        call = build(tiles, strips, slots, fields_n, levels, cells)
        wet_land, surface_diagonal = (jnp.swapaxes(x, 1, 2) for x in (wet_land, surface_diagonal))
        new, answer, left = call(fields, wet_land, links, surface_diagonal, spread, mixing, thickness)
        new, answer, left = put(new, answer, left)
        return new, jnp.swapaxes(answer, 1, 2), jnp.swapaxes(left, 1, 2)

    placed = (
        P("tiles", "strip", None, None, None, None),
        P("tiles", "strip", None, None),
        P("tiles", "strip", None, None, None),
        P("tiles", "strip", None, None),
        P(),
        P(),
        P(),
    )
    return jax.shard_map(
        on_device,
        mesh=mesh,
        in_specs=placed,
        out_specs=(
            P("tiles", "strip", None, None, None, None),
            P("tiles", "strip", None, None),
            P("tiles", "strip", None, None),
        ),
        check_vma=False,
    )
```

```python
import math

import jax
import jax.numpy as jnp
from jax import lax
from jax.experimental import pallas as pl
from jax.experimental.pallas import tpu as pltpu
from jax.sharding import PartitionSpec as P

LANES = 128
CHUNK = 1024
POS = (0, 3, 1, 2)
GROUP = 16


def offsets(size):
    return (-1, 0, 1) if size >= 3 else tuple(range(size))


def place(offset, size):
    if size >= 3:
        return offset + 1
    return offset * offset if size == 2 else 0 * offset


def roll(value, shift, axis=1):
    size = value.shape[axis]
    shift = shift % size
    return pltpu.roll(value, shift, axis) if shift else value


def build(tiles, strips, slots, fields_n, levels, cells):
    width = math.isqrt(cells)
    n_tiles = -(-cells // CHUNK) * CHUNK // LANES
    wide = n_tiles * LANES
    padded = wide + 2 * LANES
    chunks = wide // CHUNK
    steps_t, steps_s = offsets(tiles), offsets(strips)
    n_s = len(steps_s)
    n_dirs = len(steps_t) * n_s
    low = min(GROUP, tiles)
    high = tiles // low
    first = low * strips
    directions = []
    for dt in steps_t:
        for ds in steps_s:
            if dt == 0 and ds == 0:
                continue
            sides = []
            if dt == -1 or (tiles == 2 and dt):
                sides.append(0)
            if ds == -1 or (strips == 2 and ds):
                sides.append(1)
            if ds == 1:
                sides.append(2)
            if dt == 1:
                sides.append(3)
            here = place(dt, tiles) * n_s + place(ds, strips)
            back = place(-dt if tiles >= 3 else dt, tiles) * n_s + place(-ds if strips >= 3 else ds, strips)
            directions.append((dt, ds, here, back, min(sides), max(sides) + 1))

    def kernel(
        fields, wet_in, links_in, diag_in, spread_in, mixing_in, thick_in, out_f, out_x, out_r,
        links, spread, mixing, thick, fbuf, wbuf, dbuf, m_ref, w_ref, d_ref, nw_ref, ne_ref, uv_ref, s_ref, u_ref, v_ref, eb_ref, ebs_ref,
        rim_ref, rims_ref, pack1, near1, packb, nearb, pack2, near2, pack3, near3, row_ref, red_ref, red2_ref,
        in_sem, send1, recv1, sendb, recvb, send2, recv2, send3, recv3, sendr, recvr, sendq, recvq,
    ):
        t = lax.axis_index("tiles")
        s = lax.axis_index("strip")
        copies = [
            pltpu.make_async_copy(wet_in.at[0], wbuf, in_sem.at[0]),
            pltpu.make_async_copy(diag_in.at[0], dbuf, in_sem.at[1]),
        ] + [pltpu.make_async_copy(fields.at[0, 0, k], fbuf.at[k], in_sem.at[2 + k]) for k in range(slots)]
        small = [
            pltpu.make_async_copy(thick_in, thick, in_sem.at[2 + slots]),
            pltpu.make_async_copy(mixing_in, mixing, in_sem.at[3 + slots]),
            pltpu.make_async_copy(spread_in, spread, in_sem.at[4 + slots]),
            pltpu.make_async_copy(links_in.at[0, 0], links, in_sem.at[5 + slots]),
        ]
        for copy in copies[:3] + small + copies[3:]:
            copy.start()

        barrier = pltpu.get_barrier_semaphore()
        base = (t // low) * low
        place_t = t % low
        me_first = place_t * strips + s
        peers = 0
        for j in range(1, first):
            other = lax.rem(me_first + j, first)
            pl.semaphore_signal(
                barrier, inc=1, device_id=(base + other // strips, other % strips),
                device_id_type=pl.DeviceIdType.MESH,
            )
            peers += 1
        for j in range(1, high):
            other = lax.rem(t // low + j, high)
            pl.semaphore_signal(
                barrier, inc=1, device_id=(other * low + place_t, s), device_id_type=pl.DeviceIdType.MESH
            )
            peers += 1
        if high > 1:
            for dt, ds, here, back, lo, hi in directions:
                pl.semaphore_signal(
                    barrier, inc=1,
                    device_id=(lax.rem(t + dt + tiles, tiles), lax.rem(s + ds + strips, strips)),
                    device_id_type=pl.DeviceIdType.MESH,
                )
                peers += 1

        def exchange(pack, near, send_sem, recv_sem):
            out = []
            for dt, ds, here, back, lo, hi in directions:
                copy = pltpu.make_async_remote_copy(
                    src_ref=pack.at[pl.ds(lo, hi - lo)],
                    dst_ref=near.at[back, pl.ds(lo, hi - lo)],
                    send_sem=send_sem.at[here],
                    recv_sem=recv_sem.at[back],
                    device_id=(lax.rem(t + dt + tiles, tiles), lax.rem(s + ds + strips, strips)),
                    device_id_type=pl.DeviceIdType.MESH,
                )
                copy.start()
                out.append(copy)
            return out

        lane = lax.broadcasted_iota(jnp.int32, (1, LANES), 1)
        flip_at = jnp.where(lane < width, width - 1 - lane, lane)

        def flip(value):
            rows = value.shape[0]
            if rows < 8:
                value = jnp.concatenate([value, jnp.zeros((8 - rows, LANES), jnp.float32)], 0)
            at = jnp.broadcast_to(flip_at, value.shape)
            return jnp.take_along_axis(value, at, axis=1)[:rows]

        def extract(tile, rows):
            blank = jnp.zeros((rows, LANES), jnp.float32)
            parts_w, parts_e = [blank] * 4, [blank] * 4
            loaded = {}

            def at(n):
                if n not in loaded:
                    loaded[n] = tile(n)
                return loaded[n]

            for i in range(-1, width):
                pe = width * i + width - 1
                pw = pe + 1
                shift = (i - pe) % LANES
                turned = {}
                for n in {pe // LANES if i >= 0 else pw // LANES, pw // LANES if i + 1 < width else pe // LANES}:
                    turned[n] = roll(at(n), shift)
                if i >= 0:
                    parts_e[i % 4] = jnp.where(lane == i, turned[pe // LANES], parts_e[i % 4])
                if i + 1 < width:
                    parts_w[i % 4] = jnp.where(lane == i + 1, turned[pw // LANES], parts_w[i % 4])
            west = (parts_w[0] + parts_w[1]) + (parts_w[2] + parts_w[3])
            east = (parts_e[0] + parts_e[1]) + (parts_e[2] + parts_e[3])

            def line(start):
                a, n = start % LANES, start // LANES
                if a == 0:
                    return jnp.where(lane < width, at(n), 0.0)
                head = roll(at(n), -a)
                if a + width <= LANES:
                    return jnp.where(lane < width, head, 0.0)
                tail = roll(at(n + 1), -a)
                return jnp.where(lane < LANES - a, head, jnp.where(lane < width, tail, 0.0))

            return west, east, line(0), line(width * (width - 1))

        def insert(west, east, south, north, store):
            even = (lane & 1) == 0
            mixed = (jnp.where(even, east, west), jnp.where(even, west, east))
            tiles_of = {}

            def add(n, mask, value):
                tiles_of.setdefault(n, []).append((mask, value))

            for i in range(-1, width):
                pe = width * i + width - 1
                pw = pe + 1
                turned = roll(mixed[i % 2], (pe - i) % LANES)
                if i >= 0 and i + 1 < width and pe // LANES == pw // LANES:
                    mask = (lane == pe % LANES) | (lane == pw % LANES)
                    add(pe // LANES, mask, turned)
                else:
                    if i >= 0:
                        add(pe // LANES, lane == pe % LANES, turned)
                    if i + 1 < width:
                        add(pw // LANES, lane == pw % LANES, turned)
            extra = {}
            for start, rim in ((0, south), (width * (width - 1), north)):
                a, n = start % LANES, start // LANES
                turned = roll(rim, a)
                extra.setdefault(n, []).append(jnp.where(lane >= a, turned, 0.0) if a else turned)
                if a + width > LANES:
                    extra.setdefault(n + 1, []).append(jnp.where(lane < a + width - LANES, turned, 0.0))
            blank = jnp.zeros(west.shape, jnp.float32)
            for n in range(n_tiles):
                total = blank
                for mask, value in tiles_of.get(n, ()):
                    total = jnp.where(mask, value, total)
                for value in extra.get(n, ()):
                    total = total + value
                store(n, total)

        shift_bits = 22
        factor = (1 << shift_bits) // width + 1
        for c in range(chunks):
            index = lax.broadcasted_iota(jnp.int32, (1, CHUNK), 1) + c * CHUNK
            column = index - width * ((index * factor) >> shift_bits)
            nw_ref[:, pl.ds(c * CHUNK, CHUNK)] = jnp.where(column == 0, 0.0, 1.0)
            ne_ref[:, pl.ds(c * CHUNK, CHUNK)] = jnp.where(column == width - 1, 0.0, 1.0)
        tail = wide - LANES
        m_ref[:, :, :LANES] = jnp.zeros((slots * fields_n, levels, LANES), jnp.float32)
        m_ref[:, :, tail + LANES :] = jnp.zeros((slots * fields_n, levels, 2 * LANES), jnp.float32)
        uv_ref[:, :, :LANES] = jnp.zeros((2, slots, LANES), jnp.float32)
        uv_ref[:, :, tail + LANES :] = jnp.zeros((2, slots, 2 * LANES), jnp.float32)
        for ref in (s_ref, u_ref):
            ref[:, :LANES] = jnp.zeros((slots, LANES), jnp.float32)
            ref[:, wide + LANES :] = jnp.zeros((slots, LANES), jnp.float32)
        w_ref[:, tail:] = jnp.zeros((slots, LANES), jnp.float32)
        d_ref[:, tail:] = jnp.zeros((slots, LANES), jnp.float32)

        def per_level(read):
            level = lax.broadcasted_iota(jnp.int32, (levels, 1), 0)
            value = jnp.zeros((levels, 1), jnp.float32)
            for n in range(levels):
                value = jnp.where(level == n, read(n), value)
            return value

        for copy in small:
            copy.wait()
        thick_col = per_level(lambda n: thick[n])
        mix_col = per_level(lambda n: mixing[n])

        copies[0].wait()
        copies[1].wait()
        spans = [(c * CHUNK, min(CHUNK, cells - c * CHUNK)) for c in range(chunks)]
        for k in range(slots):
            for at, size in spans:
                w_ref[k : k + 1, pl.ds(at, size)] = wbuf[k, :, pl.ds(at, size)].astype(jnp.float32)
                d_ref[k : k + 1, pl.ds(at, size)] = dbuf[k, :, pl.ds(at, size)] + 4.0
        for k in range(slots):
            copies[2 + k].wait()
            for f in range(fields_n):
                for at, size in spans:
                    masked = fbuf[k, f, :, pl.ds(at, size)] * w_ref[k : k + 1, pl.ds(at, size)]
                    m_ref[k * fields_n + f, :, pl.ds(LANES + at, size)] = masked
                    if f < 2:
                        uv_ref[f, k : k + 1, pl.ds(LANES + at, size)] = jnp.sum(
                            masked * thick_col, axis=0, keepdims=True
                        )

        for f in range(2):
            for e, rim in enumerate(extract(lambda n: uv_ref[f, :, pl.ds(LANES * (n + 1), LANES)], slots)):
                for k in range(slots):
                    pack1[POS[e], k, f : f + 1, :] = rim[k : k + 1]

        pl.semaphore_wait(barrier, peers)
        sent1 = exchange(pack1, near1, send1, recv1)

        def slab_pack(kf, carry):
            rims = extract(lambda n: m_ref[kf, :, pl.ds(LANES * (n + 1), LANES)], levels)
            for e, rim in enumerate(rims):
                packb[POS[e], kf] = rim
            return carry

        lax.fori_loop(0, slots * fields_n, slab_pack, 0)
        sentb = exchange(packb, nearb, sendb, recvb)

        def entry(k, e):
            dt, ds, p, code = (links[k, e, n] for n in range(4))
            source = place(dt, tiles) * n_s + place(ds, strips)
            return source, jnp.maximum(p, 0), p, code

        def choose(number, test, yes, no):
            return jnp.where(test(jnp.full(yes.shape, number, jnp.int32)), yes, no)

        def turn(code):
            a = jnp.where(code == 0, 1.0, jnp.where(code == 2, -1.0, 0.0))
            b = jnp.where(code == 1, 1.0, jnp.where(code == 3, -1.0, 0.0))
            return a, b

        def surface_rims(near):
            for e in range(4):
                for k in range(slots):
                    source, slot, p, code = entry(k, e)
                    rim = near[source, POS[e ^ 1], slot]
                    rim = choose(code, lambda x: x != 0, flip(rim), rim)
                    rim_ref[e, k : k + 1, :] = choose(p, lambda x: x >= 0, rim, jnp.zeros_like(rim))

        def put_edges():
            def store(n, value):
                eb_ref[:, pl.ds(n * LANES, LANES)] = value

            insert(rim_ref[0], rim_ref[1], rim_ref[2], rim_ref[3], store)

        def side_totals():
            west, east, south, north = (rim_ref[e] for e in range(4))
            end = slice(width - 1, width)

            def ends(at_first, at_last):
                return jnp.where(lane == 0, at_first, jnp.where(lane == width - 1, at_last, 0.0))

            return (
                west + ends(south[:, :1], north[:, :1]),
                east + ends(south[:, end], north[:, end]),
                south + ends(west[:, :1], east[:, :1]),
                north + ends(west[:, end], east[:, end]),
            )

        def send_rims(rims, pack, near, send_sem, recv_sem):
            for e, rim in enumerate(rims):
                for k in range(slots):
                    pack[POS[e], k, :, :] = rim[k : k + 1]
            return exchange(pack, near, send_sem, recv_sem)

        def rims_of(x_ref, lead):
            return extract(lambda n: x_ref[:, pl.ds(LANES * n + lead, LANES)], slots)

        inner = slice(LANES, LANES + CHUNK)

        def image(x_ref, at):
            span = pl.ds(at, CHUNK)
            win = x_ref[:, pl.ds(at, CHUNK + 2 * LANES)]
            near = ne_ref[:, span] * roll(win, -1)[:, inner] + nw_ref[:, span] * roll(win, 1)[:, inner]
            near = near + (roll(win, -width)[:, inner] + roll(win, width)[:, inner])
            return w_ref[:, span] * (d_ref[:, span] * win[:, inner] - near)

        def slab_slot(k):
            for e in range(4):
                source, slot, p, code = entry(k, e)
                a, b = turn(code)
                got = []
                for f in range(fields_n):
                    rim = nearb[source, POS[e ^ 1], slot * fields_n + f]
                    rim = choose(code, lambda x: x != 0, flip(rim), rim)
                    got.append(choose(p, lambda x: x >= 0, rim, jnp.zeros_like(rim)))
                rims_ref[e, 0] = a * got[0] + b * got[1]
                rims_ref[e, 1] = a * got[1] - b * got[0]
                for f in range(2, fields_n):
                    rims_ref[e, f] = got[f]

            def one(f, carry):
                def store(n, value):
                    ebs_ref[:, pl.ds(n * LANES, LANES)] = value

                insert(rims_ref[0, f], rims_ref[1, f], rims_ref[2, f], rims_ref[3, f], store)
                spread_col = per_level(lambda n: spread[f, n])
                for at, size in spans:
                    span = pl.ds(at, CHUNK)
                    win = m_ref[k * fields_n + f, :, pl.ds(at, CHUNK + 2 * LANES)]
                    mid = win[:, inner]
                    flat = ne_ref[:, span] * roll(win, -1)[:, inner] + nw_ref[:, span] * roll(win, 1)[:, inner]
                    flat = flat + (roll(win, -width)[:, inner] + roll(win, width)[:, inner]) + ebs_ref[:, span]
                    flat = flat - 4.0 * mid
                    above = jnp.concatenate([mid[1:], mid[-1:]], 0)
                    below = jnp.concatenate([mid[:1], mid[:-1]], 0)
                    column = above + below - 2.0 * mid
                    new = w_ref[k : k + 1, span] * (mid + spread_col * flat + mix_col * column)
                    out_f[0, 0, k, f, :, pl.ds(at, size)] = new[:, :size]
                return carry

            lax.fori_loop(0, fields_n, one, 0)

        def slab_part(part):
            for k in range(slots):
                if k * 3 // slots == part:
                    slab_slot(k)

        wet_rims = rims_of(w_ref, 0)
        for c in range(chunks):
            at = c * CHUNK
            span = pl.ds(at, CHUNK)
            u_win = uv_ref[0, :, pl.ds(at, CHUNK + 2 * LANES)]
            v_win = uv_ref[1, :, pl.ds(at, CHUNK + 2 * LANES)]
            flux = ne_ref[:, span] * roll(u_win, -1)[:, inner] - nw_ref[:, span] * roll(u_win, 1)[:, inner]
            flux = flux + (roll(v_win, -width)[:, inner] - roll(v_win, width)[:, inner])
            s_ref[:, pl.ds(LANES + at, CHUNK)] = w_ref[:, span] * (0.5 * flux)
        own = rims_of(s_ref, LANES)

        for copy in sent1:
            copy.wait_recv()
        for e in range(4):
            for k in range(slots):
                source, slot, p, code = entry(k, e)
                pair = near1[source, POS[e ^ 1], slot]
                pair = choose(code, lambda x: x != 0, flip(pair), pair)
                pair = choose(p, lambda x: x >= 0, pair, jnp.zeros_like(pair))
                a, b = turn(code)
                if e < 2:
                    rim = a * pair[0:1] + b * pair[1:2]
                else:
                    rim = a * pair[1:2] - b * pair[0:1]
                rim_ref[e, k : k + 1, :] = (0.5 if e in (1, 3) else -0.5) * rim
        s_rims = [x + w * y for x, w, y in zip(own, wet_rims, side_totals())]
        sent2 = send_rims(s_rims, pack2, near2, send2, recv2)

        put_edges()
        for c in range(chunks):
            span, shifted = pl.ds(c * CHUNK, CHUNK), pl.ds(LANES + c * CHUNK, CHUNK)
            s_ref[:, shifted] = s_ref[:, shifted] + w_ref[:, span] * eb_ref[:, span]
        for c in range(chunks):
            u_ref[:, pl.ds(LANES + c * CHUNK, CHUNK)] = image(s_ref, c * CHUNK)
        own = rims_of(u_ref, LANES)
        for copy in sentb:
            copy.wait_recv()
        slab_part(0)

        for copy in sent2:
            copy.wait_recv()
        surface_rims(near2)
        u_rims = [x - w * y for x, w, y in zip(own, wet_rims, side_totals())]
        sent3 = send_rims(u_rims, pack3, near3, send3, recv3)

        put_edges()
        for c in range(chunks):
            span, shifted = pl.ds(c * CHUNK, CHUNK), pl.ds(LANES + c * CHUNK, CHUNK)
            u_ref[:, shifted] = u_ref[:, shifted] - w_ref[:, span] * eb_ref[:, span]
        blank = jnp.zeros((slots, CHUNK), jnp.float32)

        def whole(value):
            return jnp.sum(jnp.sum(value, axis=1, keepdims=True), axis=0, keepdims=True)

        ss = su = uu = uv = blank
        for c in range(chunks):
            x = s_ref[:, pl.ds(LANES + c * CHUNK, CHUNK)]
            y = u_ref[:, pl.ds(LANES + c * CHUNK, CHUNK)]
            z = image(u_ref, c * CHUNK)
            v_ref[:, pl.ds(c * CHUNK, CHUNK)] = z
            ss, su, uu, uv = ss + x * x, su + x * y, uu + y * y, uv + y * z
        ss, su, uu, uv = whole(ss), whole(su), whole(uu), whole(uv)
        ratio = jnp.where(su > 0.0, ss / su, 0.0)
        ee = eu = ef = uf = blank
        for c in range(chunks):
            x = s_ref[:, pl.ds(LANES + c * CHUNK, CHUNK)]
            y = u_ref[:, pl.ds(LANES + c * CHUNK, CHUNK)]
            z = v_ref[:, pl.ds(c * CHUNK, CHUNK)]
            left = x - ratio * y
            left_image = y - ratio * z
            ee, eu, ef = ee + left * left, eu + left * y, ef + left * left_image
            uf = uf + (y * left_image + left * z)
        row = jnp.zeros((1, LANES), jnp.float32)
        for n, value in enumerate((ss, su, ratio, whole(ee), whole(eu), uu, whole(ef), whole(uf), uv)):
            row = jnp.where(lane == n, value, row)
        slab_part(1)

        for copy in sent3:
            copy.wait_recv()
        surface_rims(near3)
        edge_u = edge_left = jnp.zeros((slots, LANES), jnp.float32)
        for e in range(4):
            got = rim_ref[e]
            edge_u = edge_u + u_rims[e] * got
            edge_left = edge_left + (s_rims[e] - ratio * u_rims[e]) * got
        edge_u, edge_left = whole(edge_u), whole(edge_left)
        row = row + jnp.where(
            lane == 6, ratio * edge_left,
            jnp.where(lane == 7, ratio * edge_u - edge_left, jnp.where(lane == 8, -edge_u, 0.0)),
        )
        row_ref[...] = row
        red_ref[me_first] = row

        def first_copy(j):
            other = lax.rem(me_first + j, first)
            return pltpu.make_async_remote_copy(
                src_ref=row_ref,
                dst_ref=red_ref.at[me_first],
                send_sem=sendr.at[j],
                recv_sem=recvr.at[me_first],
                device_id=(base + other // strips, other % strips),
                device_id_type=pl.DeviceIdType.MESH,
            )

        def first_arrival(j):
            other = lax.rem(me_first + j, first)
            return pltpu.make_async_remote_copy(
                src_ref=row_ref,
                dst_ref=red_ref.at[other],
                send_sem=sendr.at[j],
                recv_sem=recvr.at[other],
                device_id=(base + other // strips, other % strips),
                device_id_type=pl.DeviceIdType.MESH,
            )

        for j in sorted(range(1, first), key=lambda j: abs(2 * j - first)):
            first_copy(j).start()
        put_edges()
        for c in range(chunks):
            span = pl.ds(c * CHUNK, CHUNK)
            v_ref[:, span] = v_ref[:, span] - w_ref[:, span] * eb_ref[:, span]
        slab_part(2)
        for j in range(1, first):
            first_arrival(j).wait_recv()

        if high > 1:
            mine = t // low
            copies2 = []
            for j in range(1, high):
                other = lax.rem(mine + j, high)
                copy = pltpu.make_async_remote_copy(
                    src_ref=red_ref,
                    dst_ref=red2_ref.at[mine],
                    send_sem=sendq.at[j],
                    recv_sem=recvq.at[mine],
                    device_id=(other * low + place_t, s),
                    device_id_type=pl.DeviceIdType.MESH,
                )
                copy.start()
                copies2.append(copy)
            red2_ref[mine] = red_ref[...]
            for j in range(1, high):
                other = lax.rem(mine + j, high)
                pltpu.make_async_remote_copy(
                    src_ref=red_ref,
                    dst_ref=red2_ref.at[other],
                    send_sem=sendq.at[j],
                    recv_sem=recvq.at[other],
                    device_id=(other * low + place_t, s),
                    device_id_type=pl.DeviceIdType.MESH,
                ).wait_recv()
            for copy in copies2:
                copy.wait_send()
            rows = [red2_ref[n] for n in range(high)]
        else:
            rows = [red_ref[...]]

        total = sum(jnp.sum(x, axis=0) for x in rows)
        rr0, sas = total[:, 0:1], total[:, 1:2]
        alpha0 = rr0 / sas
        moved = jnp.zeros((1, LANES), jnp.float32)
        lane3 = lax.broadcasted_iota(jnp.int32, (1, 1, LANES), 2)
        for x in rows:
            delta = jnp.broadcast_to(x[:, :, 2:3], x.shape) - alpha0[None]
            weight = jnp.where(
                (lane3 == 3) | (lane3 == 6), 1.0,
                jnp.where(lane3 == 4, 2.0 * delta, jnp.where(lane3 == 7, delta, delta * delta)),
            )
            moved = moved + jnp.sum(x * weight, axis=0)
        rr1 = jnp.sum(jnp.where((lane >= 3) & (lane <= 5), moved, 0.0), axis=1, keepdims=True)
        rar = jnp.sum(jnp.where((lane >= 6) & (lane <= 8), moved, 0.0), axis=1, keepdims=True)
        beta = rr1 / rr0
        alpha1 = rr1 / (rar - beta * rr1 / alpha0)
        for at, size in spans:
            x = s_ref[:, pl.ds(LANES + at, CHUNK)]
            y = u_ref[:, pl.ds(LANES + at, CHUNK)]
            z = v_ref[:, pl.ds(at, CHUNK)]
            r1 = x - alpha0 * y
            direction = r1 + beta * x
            direction_image = (y - alpha0 * z) + beta * y
            answer = alpha0 * x + alpha1 * direction
            left = r1 - alpha1 * direction_image
            for k in range(slots):
                out_x[0, k, :, pl.ds(at, size)] = answer[k : k + 1, :size]
                out_r[0, k, :, pl.ds(at, size)] = left[k : k + 1, :size]

        for copy in sent1 + sentb + sent2 + sent3:
            copy.wait_send()
        for j in range(1, first):
            first_copy(j).wait_send()

    f32 = jnp.float32
    any_space = pl.BlockSpec(memory_space=pl.ANY)
    hbm = pl.BlockSpec(memory_space=pltpu.HBM)
    vmem = pl.BlockSpec(memory_space=pltpu.VMEM)
    kf = slots * fields_n
    dma = pltpu.SemaphoreType.DMA
    return pl.pallas_call(
        kernel,
        out_shape=(
            pltpu.VMEM((1, 1, slots, fields_n, levels, cells), f32),
            pltpu.VMEM((1, slots, 1, cells), f32),
            pltpu.VMEM((1, slots, 1, cells), f32),
        ),
        in_specs=[hbm] * 7,
        out_specs=(vmem, vmem, vmem),
        scratch_shapes=[
            pltpu.SMEM((slots, 4, 4), jnp.int32),
            pltpu.SMEM((fields_n, levels), f32),
            pltpu.SMEM((levels,), f32),
            pltpu.SMEM((levels,), f32),
            pltpu.VMEM((slots, fields_n, levels, cells), f32),
            pltpu.VMEM((slots, 1, cells), jnp.int32),
            pltpu.VMEM((slots, 1, cells), f32),
            pltpu.VMEM((kf, levels, padded), f32),
            pltpu.VMEM((slots, wide), f32),
            pltpu.VMEM((slots, wide), f32),
            pltpu.VMEM((1, wide), f32),
            pltpu.VMEM((1, wide), f32),
            pltpu.VMEM((2, slots, padded), f32),
            pltpu.VMEM((slots, padded), f32),
            pltpu.VMEM((slots, padded), f32),
            pltpu.VMEM((slots, wide), f32),
            pltpu.VMEM((slots, wide), f32),
            pltpu.VMEM((levels, wide), f32),
            pltpu.VMEM((4, slots, LANES), f32),
            pltpu.VMEM((4, fields_n, levels, LANES), f32),
            pltpu.VMEM((4, slots, 2, LANES), f32),
            pltpu.VMEM((n_dirs, 4, slots, 2, LANES), f32),
            pltpu.VMEM((4, kf, levels, LANES), f32),
            pltpu.VMEM((n_dirs, 4, kf, levels, LANES), f32),
            pltpu.VMEM((4, slots, 1, LANES), f32),
            pltpu.VMEM((n_dirs, 4, slots, 1, LANES), f32),
            pltpu.VMEM((4, slots, 1, LANES), f32),
            pltpu.VMEM((n_dirs, 4, slots, 1, LANES), f32),
            pltpu.VMEM((1, LANES), f32),
            pltpu.VMEM((first, 1, LANES), f32),
            pltpu.VMEM((high, first, 1, LANES) if high > 1 else (1, 1, 1, LANES), f32),
            dma((6 + slots,)),
            dma((n_dirs,)), dma((n_dirs,)), dma((n_dirs,)), dma((n_dirs,)),
            dma((n_dirs,)), dma((n_dirs,)), dma((n_dirs,)), dma((n_dirs,)),
            dma((first,)), dma((first,)), dma((high,)), dma((high,)),
        ],
        compiler_params=pltpu.CompilerParams(
            collective_id=0, has_side_effects=True, vmem_limit_bytes=58 << 20
        ),
    )


def put(*arrays):
    def kernel(*refs):
        count = len(arrays)
        sems = refs[-1]
        copies = [pltpu.make_async_copy(refs[n], refs[count + n], sems.at[n]) for n in range(count)]
        for copy in copies:
            copy.start()
        for copy in copies:
            copy.wait()

    return pl.pallas_call(
        kernel,
        out_shape=tuple(jax.ShapeDtypeStruct(x.shape, x.dtype) for x in arrays),
        in_specs=[pl.BlockSpec(memory_space=pl.ANY)] * len(arrays),
        out_specs=tuple(pl.BlockSpec(memory_space=pltpu.HBM) for _ in arrays),
        scratch_shapes=[pltpu.SemaphoreType.DMA((len(arrays),))],
        compiler_params=pltpu.CompilerParams(vmem_limit_bytes=1 << 20),
    )(*arrays)


def solution(mesh):
    tiles, strips = mesh.shape["tiles"], mesh.shape["strip"]

    def on_device(fields, wet_land, links, surface_diagonal, spread, mixing, thickness):
        slots, fields_n, levels, cells = fields.shape[2:]
        call = build(tiles, strips, slots, fields_n, levels, cells)
        wet_land, surface_diagonal = (jnp.swapaxes(x, 1, 2) for x in (wet_land, surface_diagonal))
        new, answer, left = call(fields, wet_land, links, surface_diagonal, spread, mixing, thickness)
        new, answer, left = put(new, answer, left)
        return new, jnp.swapaxes(answer, 1, 2), jnp.swapaxes(left, 1, 2)

    placed = (
        P("tiles", "strip", None, None, None, None),
        P("tiles", "strip", None, None),
        P("tiles", "strip", None, None, None),
        P("tiles", "strip", None, None),
        P(),
        P(),
        P(),
    )
    return jax.shard_map(
        on_device,
        mesh=mesh,
        in_specs=placed,
        out_specs=(
            P("tiles", "strip", None, None, None, None),
            P("tiles", "strip", None, None),
            P("tiles", "strip", None, None),
        ),
        check_vma=False,
    )
```
